16 devices in a mesh: rep: 1, dp: 16 (over x, y, z, core).
Axes of the slice: x: 2, y: 2, z: 2, core: 2. Of those that a mesh axis runs over, the one named last changes fastest.
Arguments:
- a: bfloat16 [16, 4, 4096, 640], P(('rep', 'dp'))
- g: bfloat16 [16, 4, 4096, 4096], P(('rep', 'dp'))
Outputs:
- output: bfloat16 [4, 640, 4096], P('rep')
All inputs are finite; a program needn't handle non-finite values.
Results may differ from the reference program's by a relative error of at most 0.012.
Values are sent between devices in bfloat16 or wider.
A program may use at most 2 GiB of HBM per device.

```python
import jax
import jax.numpy as jnp
from jax import lax

DEVICES = 16
MATRICES = 4
TOKENS = 4096
D = 640
FF = 4096


def setup_inputs(seed: int = 0, part: int = 0) -> dict:
    ka, kg, ks = (jax.random.fold_in(k, part) for k in jax.random.split(jax.random.key(seed), 3))
    size = 2.0 ** jax.random.uniform(ks, (DEVICES, MATRICES, 1, 1), jnp.float32, -1.0, 1.0)
    a = jax.random.normal(ka, (DEVICES, MATRICES, TOKENS, D), jnp.float32)
    g = size * jax.random.normal(kg, (DEVICES, MATRICES, TOKENS, FF), jnp.float32) * (DEVICES * TOKENS) ** -0.5
    return {"a": a.astype(jnp.bfloat16), "g": g.astype(jnp.bfloat16)}


def reference(a, g):
    def take(so_far, one):
        return so_far + jnp.einsum("ntd,ntf->ndf", *one, preferred_element_type=jnp.float32), None

    return lax.scan(take, jnp.zeros((MATRICES, D, FF), jnp.float32), (a, g))[0].astype(jnp.bfloat16)
```

```python
import functools

import jax
import jax.numpy as jnp
from jax import lax
from jax.experimental import pallas as pl
from jax.experimental.pallas import tpu as pltpu

MESH = pl.DeviceIdType.MESH
F32 = jnp.float32
BF16 = jnp.bfloat16

W = 512
UW = 256
KBLOCKS = 8
GSLOTS = 3
SLOTS = 8
LAGS = (2, 4, 8, 12, 16, 20)


def kernel(a_ref, g_ref, o_ref, at, stage, gbuf, acc, keep0, keep1, keep2,
           sbuf0, sbuf1, sbuf2, sbuf3, stage_sem, g_sem, send_sem, recv_sem, free_sem):
    matrices, tokens, d = a_ref.shape[1:]
    f = g_ref.shape[3]
    kb = tokens // KBLOCKS
    per = f // W
    chunks = matrices * per
    units = chunks * (W // UW)
    uper = f // UW

    me = lax.axis_index("dp")
    core = lax.rem(me, 2)
    z = lax.rem(me // 2, 2)
    y = lax.rem(me // 4, 2)
    x = lax.rem(me // 8, 2)
    other = me + 1 - 2 * core

    def bit_of(dim):
        return jnp.where(dim == 0, x, jnp.where(dim == 1, y, z))

    def peer_of(dim):
        b = bit_of(dim)
        step = jnp.where(dim == 0, 8, jnp.where(dim == 1, 4, 2))
        return me + step * (1 - 2 * b)

    def dims(u):
        r = lax.rem(u, 3)
        return r, lax.rem(r + 1, 3), lax.rem(r + 2, 3)

    def rows(u):
        d0, d1, d2 = dims(u)
        h1, h2, h3 = d // 2, d // 4, d // 8
        b0, b1, b2 = bit_of(d0), bit_of(d1), bit_of(d2)
        k1, s1 = b0 * h1, (1 - b0) * h1
        k2, s2 = k1 + b1 * h2, k1 + (1 - b1) * h2
        k3, s3 = k2 + b2 * h3, k2 + (1 - b2) * h3
        return (k1, k2, k3), (s1, s2, s3)

    def rds(start, size):
        return pl.ds(pl.multiple_of(start, 16), size)

    def cols(u, c):
        return pl.ds(pl.multiple_of(lax.rem(u, uper) * UW + c * 128, 128), 128)

    def mine(u):
        return u // uper, cols(u, core)

    def theirs(u):
        return u // uper, cols(u, 1 - core)

    def remote(src, dst, stage_no, u, device):
        return pltpu.make_async_remote_copy(
            src, dst, send_sem.at[stage_no, u], recv_sem.at[stage_no, u],
            device_id={"dp": device}, device_id_type=MESH)

    h1, h2, h3 = d // 2, d // 4, d // 8

    def core_reduce(u):
        n, c = mine(u)
        no, co = theirs(u)
        return remote(sbuf0.at[lax.rem(u, SLOTS)], o_ref.at[no, :, co], 0, u, other)

    def chip_reduce(u, s):
        n, c = theirs(u)
        dim = dims(u)[s]
        buf = (sbuf1, sbuf2, sbuf3)[s]
        start, size = ((0, h1), (h1, h2), (h1 + h2, h3))[s]
        return remote(buf.at[lax.rem(u, SLOTS)], o_ref.at[n, pl.ds(start, size), c], 1 + s, u, peer_of(dim))

    def chip_gather(u, s):
        n, c = mine(u)
        dim = dims(u)[2 - s]
        start = rows(u)[0][2 - s]
        size = (h3, h2, h1)[s]
        ref = o_ref.at[n, rds(start, size), c]
        return remote(ref, ref, 4 + s, u, peer_of(dim))

    def core_gather(u):
        n, c = mine(u)
        ref = o_ref.at[n, :, c]
        return remote(ref, ref, 7, u, other)

    def landed(ref, stage_no, u):
        pltpu.make_async_copy(ref, ref, recv_sem.at[stage_no, u]).wait()

    def left(ref, stage_no, u):
        pltpu.make_async_copy(ref, ref, send_sem.at[stage_no, u]).wait()

    def g_copy(j):
        n = j // per
        c = pl.ds(pl.multiple_of(lax.rem(j, per) * W, W), W)
        slot = lax.rem(j, GSLOTS)
        return pltpu.make_async_copy(g_ref.at[0, n, :, c], gbuf.at[slot], g_sem.at[slot])

    def a_copy(n, k):
        return pltpu.make_async_copy(
            a_ref.at[0, n, pl.ds(pl.multiple_of(k * kb, kb), kb), :], stage.at[k], stage_sem.at[k])

    def turn(n, k):
        at[lax.rem(n, 2), :, pl.ds(pl.multiple_of(k * kb, kb), kb)] = stage[k].T

    barrier = pltpu.get_barrier_semaphore()
    peers = [other] + [peer_of(i) for i in range(3)]
    for p in peers:
        pl.semaphore_signal(barrier, inc=1, device_id={"dp": p}, device_id_type=MESH)
    pl.semaphore_wait(barrier, len(peers))

    for k in range(KBLOCKS):
        a_copy(0, k).start()
    g_copy(0).start()
    g_copy(1).start()
    for k in range(KBLOCKS):
        a_copy(0, k).wait()
        turn(0, k)

    def matmul(j):
        n = j // per
        k = lax.rem(j, per)

        @pl.when(j + 2 < chunks)
        def _():
            g_copy(j + 2).start()

        more = n + 1 < matrices

        @pl.when(more & (k == 0))
        def _():
            for i in range(KBLOCKS):
                a_copy(n + 1, i).start()

        g_copy(j).wait()
        slot = lax.rem(j, 4)
        acc[slot] = jnp.dot(at[lax.rem(n, 2)], gbuf[lax.rem(j, GSLOTS)], preferred_element_type=F32)

        for i in range(W // UW):
            u = j * (W // UW) + i

            @pl.when(u >= SLOTS)
            def _():
                core_reduce(u - SLOTS).wait_send()

            c = pl.ds(pl.multiple_of(i * UW + (1 - core) * 128, 128), 128)
            sbuf0[lax.rem(u, SLOTS)] = acc[slot, :, c].astype(BF16)
            core_reduce(u).start()

        @pl.when(more)
        def _():
            a_copy(n + 1, k).wait()
            turn(n + 1, k)

    def halve(u, s, value):
        (k1, k2, k3), (s1, s2, s3) = rows(u)
        slot = lax.rem(u, SLOTS)

        @pl.when(u >= SLOTS)
        def _():
            chip_reduce(u - SLOTS, s).wait_send()

        buf = (sbuf1, sbuf2, sbuf3)[s]
        keep = (keep0, keep1, keep2)[s]
        size = (h1, h2, h3)[s]
        b = bit_of(dims(u)[s])
        buf[slot] = value((1 - b) * size, size).astype(BF16)
        chip_reduce(u, s).start()
        keep[slot] = value(b * size, size)

    def step1(u):
        core_reduce(u).wait_recv()
        n, c = mine(u)
        aslot = lax.rem(u // 2, 4)
        ac = pl.ds(pl.multiple_of(lax.rem(u, 2) * UW + core * 128, 128), 128)

        def value(start, size):
            return acc[aslot, rds(start, size), ac] + o_ref[n, rds(start, size), c].astype(F32)

        halve(u, 0, value)

    def step23(u, s):
        chip_reduce(u, s - 1).wait_recv()
        n, c = theirs(u)
        slot = lax.rem(u, SLOTS)
        keep = (keep0, keep1)[s - 1]
        base = (0, h1)[s - 1]

        def value(start, size):
            return keep[slot, rds(start, size), :] + o_ref[n, rds(base + start, size), c].astype(F32)

        halve(u, s, value)

    def step4(u):
        chip_reduce(u, 2).wait_recv()
        n, c = theirs(u)
        slot = lax.rem(u, SLOTS)
        total = keep2[slot] + o_ref[n, pl.ds(h1 + h2, h3), c].astype(F32)
        n, c = mine(u)
        o_ref[n, rds(rows(u)[0][2], h3), c] = total.astype(BF16)
        chip_gather(u, 0).start()
        pl.semaphore_signal(free_sem, inc=1, device_id={"dp": other}, device_id_type=MESH)

    def step5(u):
        chip_gather(u, 0).wait_recv()
        chip_gather(u, 1).start()

    def step6(u):
        chip_gather(u, 1).wait_recv()
        chip_gather(u, 2).start()

    def step7(u):
        chip_gather(u, 2).wait_recv()
        pl.semaphore_wait(free_sem, 1)
        core_gather(u).start()

    steps = (step1, lambda u: step23(u, 1), lambda u: step23(u, 2), step4, step5)

    def slot(t, _):
        @pl.when(t < chunks)
        def _():
            matmul(t)

        for lag, step in zip(LAGS, steps):
            for i in range(2):
                u = 2 * t + i - lag

                @pl.when((u >= 0) & (u < units))
                def _():
                    step(u)
        lo, hi = sched6(t), sched6(t + 1)
        lax.fori_loop(lo, hi, lambda u, _: (step6(u), 0)[1], 0)
        lo, hi = sched7(t), sched7(t + 1)
        lax.fori_loop(lo, hi, lambda u, _: (step7(u), 0)[1], 0)
        return 0

    def clip(v):
        return jnp.minimum(jnp.maximum(v, 0), units)

    def sched6(t):
        return clip(2 * t - LAGS[5])

    def sched7(t):
        return clip(2 * t - LAGS[5] - 6)

    slots = (units + LAGS[5] + 6) // 2
    lax.fori_loop(0, slots, slot, 0)

    def finish(u, _):
        core_gather(u).wait_send()
        core_gather(u).wait_recv()
        for s in range(3):
            chip_gather(u, s).wait_send()
        return 0

    lax.fori_loop(0, units, finish, 0)

    def drain(u, _):
        core_reduce(u).wait_send()
        for s in range(3):
            chip_reduce(u, s).wait_send()
        return 0

    lax.fori_loop(units - SLOTS, units, drain, 0)


def solution(mesh):
    def body(a, g):
        _, n, tokens, d = a.shape
        f = g.shape[3]
        units = n * f // UW
        return pl.pallas_call(
            kernel,
            out_shape=pltpu.VMEM((n, d, f), BF16),
            in_specs=[pl.BlockSpec(memory_space=pl.ANY)] * 2,
            out_specs=pl.BlockSpec(memory_space=pltpu.VMEM),
            scratch_shapes=[
                pltpu.VMEM((2, d, tokens), BF16),
                pltpu.VMEM((KBLOCKS, tokens // KBLOCKS, d), BF16),
                pltpu.VMEM((GSLOTS, tokens, W), BF16),
                pltpu.VMEM((4, d, W), F32),
                pltpu.VMEM((SLOTS, d // 2, 128), F32),
                pltpu.VMEM((SLOTS, d // 4, 128), F32),
                pltpu.VMEM((SLOTS, d // 8, 128), F32),
                pltpu.VMEM((SLOTS, d, 128), BF16),
                pltpu.VMEM((SLOTS, d // 2, 128), BF16),
                pltpu.VMEM((SLOTS, d // 4, 128), BF16),
                pltpu.VMEM((SLOTS, d // 8, 128), BF16),
                pltpu.SemaphoreType.DMA((KBLOCKS,)),
                pltpu.SemaphoreType.DMA((GSLOTS,)),
                pltpu.SemaphoreType.DMA((8, units)),
                pltpu.SemaphoreType.DMA((8, units)),
                pltpu.SemaphoreType.REGULAR,
            ],
            compiler_params=pltpu.CompilerParams(
                collective_id=0, has_side_effects=True, vmem_limit_bytes=43 * 2**20),
        )(a, g)

    spec = jax.sharding.PartitionSpec
    return jax.shard_map(
        body, mesh=mesh, in_specs=(spec(("rep", "dp")), spec(("rep", "dp"))), out_specs=spec("rep"), check_vma=False)
```

```python
import functools

import jax
import jax.numpy as jnp
from jax import lax
from jax.experimental import pallas as pl
from jax.experimental.pallas import tpu as pltpu

MESH = pl.DeviceIdType.MESH
F32 = jnp.float32
BF16 = jnp.bfloat16

W = 512
UW = 512
KBLOCKS = 8
GSLOTS = 3
SLOTS = 4
LAGS = (1, 3, 5, 7, 9, 11)


def kernel(a_ref, g_ref, o_ref, at, stage, gbuf, acc, keep0, keep1, keep2,
           sbuf0, sbuf1, sbuf2, sbuf3, stage_sem, g_sem, send_sem, recv_sem, free_sem):
    matrices, tokens, d = a_ref.shape[1:]
    f = g_ref.shape[3]
    kb = tokens // KBLOCKS
    per = f // W
    chunks = matrices * per
    units = chunks * (W // UW)
    uper = f // UW

    me = lax.axis_index("dp")
    core = lax.rem(me, 2)
    z = lax.rem(me // 2, 2)
    y = lax.rem(me // 4, 2)
    x = lax.rem(me // 8, 2)
    other = me + 1 - 2 * core

    def bit_of(dim):
        return jnp.where(dim == 0, x, jnp.where(dim == 1, y, z))

    def peer_of(dim):
        b = bit_of(dim)
        step = jnp.where(dim == 0, 8, jnp.where(dim == 1, 4, 2))
        return me + step * (1 - 2 * b)

    def dims(u):
        r = lax.rem(u, 3)
        return r, lax.rem(r + 1, 3), lax.rem(r + 2, 3)

    def rows(u):
        d0, d1, d2 = dims(u)
        h1, h2, h3 = d // 2, d // 4, d // 8
        b0, b1, b2 = bit_of(d0), bit_of(d1), bit_of(d2)
        k1, s1 = b0 * h1, (1 - b0) * h1
        k2, s2 = k1 + b1 * h2, k1 + (1 - b1) * h2
        k3, s3 = k2 + b2 * h3, k2 + (1 - b2) * h3
        return (k1, k2, k3), (s1, s2, s3)

    def rds(start, size):
        return pl.ds(pl.multiple_of(start, 16), size)

    def cols(u, c):
        return pl.ds(pl.multiple_of(lax.rem(u, uper) * UW + c * 256, 256), 256)

    def mine(u):
        return u // uper, cols(u, core)

    def theirs(u):
        return u // uper, cols(u, 1 - core)

    def remote(src, dst, stage_no, u, device):
        return pltpu.make_async_remote_copy(
            src, dst, send_sem.at[stage_no, u], recv_sem.at[stage_no, u],
            device_id={"dp": device}, device_id_type=MESH)

    h1, h2, h3 = d // 2, d // 4, d // 8

    def core_reduce(u):
        n, c = mine(u)
        no, co = theirs(u)
        return remote(sbuf0.at[lax.rem(u, SLOTS)], o_ref.at[no, :, co], 0, u, other)

    def chip_reduce(u, s):
        n, c = theirs(u)
        dim = dims(u)[s]
        buf = (sbuf1, sbuf2, sbuf3)[s]
        start, size = ((0, h1), (h1, h2), (h1 + h2, h3))[s]
        return remote(buf.at[lax.rem(u, SLOTS)], o_ref.at[n, pl.ds(start, size), c], 1 + s, u, peer_of(dim))

    def chip_gather(u, s):
        n, c = mine(u)
        dim = dims(u)[2 - s]
        start = rows(u)[0][2 - s]
        size = (h3, h2, h1)[s]
        ref = o_ref.at[n, rds(start, size), c]
        return remote(ref, ref, 4 + s, u, peer_of(dim))

    def core_gather(u):
        n, c = mine(u)
        ref = o_ref.at[n, :, c]
        return remote(ref, ref, 7, u, other)

    def landed(ref, stage_no, u):
        pltpu.make_async_copy(ref, ref, recv_sem.at[stage_no, u]).wait()

    def left(ref, stage_no, u):
        pltpu.make_async_copy(ref, ref, send_sem.at[stage_no, u]).wait()

    def g_copy(j):
        n = j // per
        c = pl.ds(pl.multiple_of(lax.rem(j, per) * W, W), W)
        slot = lax.rem(j, GSLOTS)
        return pltpu.make_async_copy(g_ref.at[0, n, :, c], gbuf.at[slot], g_sem.at[slot])

    def a_copy(n, k):
        return pltpu.make_async_copy(
            a_ref.at[0, n, pl.ds(pl.multiple_of(k * kb, kb), kb), :], stage.at[k], stage_sem.at[k])

    def turn(n, k):
        at[lax.rem(n, 2), :, pl.ds(pl.multiple_of(k * kb, kb), kb)] = stage[k].T

    barrier = pltpu.get_barrier_semaphore()
    peers = [other] + [peer_of(i) for i in range(3)]
    for p in peers:
        pl.semaphore_signal(barrier, inc=1, device_id={"dp": p}, device_id_type=MESH)
    pl.semaphore_wait(barrier, len(peers))

    for k in range(KBLOCKS):
        a_copy(0, k).start()
    g_copy(0).start()
    g_copy(1).start()
    for k in range(KBLOCKS):
        a_copy(0, k).wait()
        turn(0, k)

    def matmul(j):
        n = j // per
        k = lax.rem(j, per)

        @pl.when(j + 2 < chunks)
        def _():
            g_copy(j + 2).start()

        more = n + 1 < matrices

        @pl.when(more & (k == 0))
        def _():
            for i in range(KBLOCKS):
                a_copy(n + 1, i).start()

        g_copy(j).wait()
        slot = lax.rem(j, 4)
        acc[slot] = jnp.dot(at[lax.rem(n, 2)], gbuf[lax.rem(j, GSLOTS)], preferred_element_type=F32)

        for i in range(W // UW):
            u = j * (W // UW) + i

            @pl.when(u >= SLOTS)
            def _():
                core_reduce(u - SLOTS).wait_send()

            c = pl.ds(pl.multiple_of(i * UW + (1 - core) * 256, 256), 256)
            sbuf0[lax.rem(u, SLOTS)] = acc[slot, :, c].astype(BF16)
            core_reduce(u).start()

        @pl.when(more)
        def _():
            a_copy(n + 1, k).wait()
            turn(n + 1, k)

    def halve(u, s, value):
        (k1, k2, k3), (s1, s2, s3) = rows(u)
        slot = lax.rem(u, SLOTS)

        @pl.when(u >= SLOTS)
        def _():
            chip_reduce(u - SLOTS, s).wait_send()

        buf = (sbuf1, sbuf2, sbuf3)[s]
        keep = (keep0, keep1, keep2)[s]
        size = (h1, h2, h3)[s]
        b = bit_of(dims(u)[s])
        buf[slot] = value((1 - b) * size, size).astype(BF16)
        chip_reduce(u, s).start()
        keep[slot] = value(b * size, size)

    def step1(u):
        core_reduce(u).wait_recv()
        n, c = mine(u)
        aslot = lax.rem(u, 4)
        ac = pl.ds(pl.multiple_of(core * 256, 256), 256)

        def value(start, size):
            return acc[aslot, rds(start, size), ac] + o_ref[n, rds(start, size), c].astype(F32)

        halve(u, 0, value)

    def step23(u, s):
        chip_reduce(u, s - 1).wait_recv()
        n, c = theirs(u)
        slot = lax.rem(u, SLOTS)
        keep = (keep0, keep1)[s - 1]
        base = (0, h1)[s - 1]

        def value(start, size):
            return keep[slot, rds(start, size), :] + o_ref[n, rds(base + start, size), c].astype(F32)

        halve(u, s, value)

    def step4(u):
        chip_reduce(u, 2).wait_recv()
        n, c = theirs(u)
        slot = lax.rem(u, SLOTS)
        total = keep2[slot] + o_ref[n, pl.ds(h1 + h2, h3), c].astype(F32)
        n, c = mine(u)
        o_ref[n, rds(rows(u)[0][2], h3), c] = total.astype(BF16)
        chip_gather(u, 0).start()
        pl.semaphore_signal(free_sem, inc=1, device_id={"dp": other}, device_id_type=MESH)

    def step5(u):
        chip_gather(u, 0).wait_recv()
        chip_gather(u, 1).start()

    def step6(u):
        chip_gather(u, 1).wait_recv()
        chip_gather(u, 2).start()

    def step7(u):
        chip_gather(u, 2).wait_recv()
        pl.semaphore_wait(free_sem, 1)
        core_gather(u).start()

    steps = (step1, lambda u: step23(u, 1), lambda u: step23(u, 2), step4, step5)

    def slot(t, _):
        @pl.when(t < chunks)
        def _():
            matmul(t)

        for lag, step in zip(LAGS, steps):
            for i in range(1):
                u = t - lag

                @pl.when((u >= 0) & (u < units))
                def _():
                    step(u)
        lo, hi = sched6(t), sched6(t + 1)
        lax.fori_loop(lo, hi, lambda u, _: (step6(u), 0)[1], 0)
        lo, hi = sched7(t), sched7(t + 1)
        lax.fori_loop(lo, hi, lambda u, _: (step7(u), 0)[1], 0)
        return 0

    def clip(v):
        return jnp.minimum(jnp.maximum(v, 0), units)

    def sched6(t):
        return clip(t - LAGS[5])

    def sched7(t):
        return clip(t - LAGS[5] - 4)

    slots = units + LAGS[5] + 4
    lax.fori_loop(0, slots, slot, 0)

    def finish(u, _):
        core_gather(u).wait_send()
        core_gather(u).wait_recv()
        for s in range(3):
            chip_gather(u, s).wait_send()
        return 0

    lax.fori_loop(0, units, finish, 0)

    def drain(u, _):
        core_reduce(u).wait_send()
        for s in range(3):
            chip_reduce(u, s).wait_send()
        return 0

    lax.fori_loop(units - SLOTS, units, drain, 0)


def solution(mesh):
    def body(a, g):
        _, n, tokens, d = a.shape
        f = g.shape[3]
        units = n * f // UW
        return pl.pallas_call(
            kernel,
            out_shape=pltpu.VMEM((n, d, f), BF16),
            in_specs=[pl.BlockSpec(memory_space=pl.ANY)] * 2,
            out_specs=pl.BlockSpec(memory_space=pltpu.VMEM),
            scratch_shapes=[
                pltpu.VMEM((2, d, tokens), BF16),
                pltpu.VMEM((KBLOCKS, tokens // KBLOCKS, d), BF16),
                pltpu.VMEM((GSLOTS, tokens, W), BF16),
                pltpu.VMEM((4, d, W), F32),
                pltpu.VMEM((SLOTS, d // 2, 256), F32),
                pltpu.VMEM((SLOTS, d // 4, 256), F32),
                pltpu.VMEM((SLOTS, d // 8, 256), F32),
                pltpu.VMEM((SLOTS, d, 256), BF16),
                pltpu.VMEM((SLOTS, d // 2, 256), BF16),
                pltpu.VMEM((SLOTS, d // 4, 256), BF16),
                pltpu.VMEM((SLOTS, d // 8, 256), BF16),
                pltpu.SemaphoreType.DMA((KBLOCKS,)),
                pltpu.SemaphoreType.DMA((GSLOTS,)),
                pltpu.SemaphoreType.DMA((8, units)),
                pltpu.SemaphoreType.DMA((8, units)),
                pltpu.SemaphoreType.REGULAR,
            ],
            compiler_params=pltpu.CompilerParams(
                collective_id=0, has_side_effects=True, vmem_limit_bytes=43 * 2**20),
        )(a, g)

    spec = jax.sharding.PartitionSpec
    return jax.shard_map(
        body, mesh=mesh, in_specs=(spec(("rep", "dp")), spec(("rep", "dp"))), out_specs=spec("rep"), check_vma=False)
```
